32 devices in a mesh: seq: 8 (over y, x, core), tensor: 4 (over z).
Axes of the slice: x: 2, y: 2, z: 4, core: 2. Of those that a mesh axis runs over, the one named last changes fastest.
Arguments:
- streams: float32 [4, 4096, 4096], P(None, 'seq', 'tensor'), may hold values from -8 to 8
- mix_weight: float32 [24, 4, 4096], P(None, None, 'tensor'), may hold values from -0.046875 to 0.046875
- mix_bias: float32 [24], replicated, may hold values from -4 to 4
- mix_scale: float32 [3], replicated, may hold values from 1 to 2
- norm_gain: bfloat16 [4096], replicated, may hold values from 0.25 to 1.75
- gate_weight: bfloat16 [4096, 7168], P('seq', 'tensor'), may hold values from -0.09375 to 0.09375
- up_weight: bfloat16 [4096, 7168], P('seq', 'tensor'), may hold values from -0.09375 to 0.09375
- down_weight: bfloat16 [7168, 4096], P('tensor', 'seq'), may hold values from -0.0625 to 0.0625
Outputs:
- new_streams: float32 [4, 4096, 4096], P(None, 'seq', 'tensor')
The draws below stay inside these ranges and needn't reach their ends.
All inputs are finite; a program needn't handle non-finite values.
Results may differ from the reference program's by a relative error of at most 0.01.
Values may be sent and summed in bfloat16 or wider, within the bound.
A program may use at most 128 MiB of HBM per device.

```python
import jax
import jax.numpy as jnp
from jax import lax

D = 4096
FF = 7168
STREAMS = 4
SWEEPS = 20
TOK_DEV = 512
TOKENS = 4096
LOGITS = 24
N_SEQ = 8
N_TENSOR = 4


def draw_streams(key, part):
    first = jax.random.fold_in(key, 11)
    second = jax.random.fold_in(key, 12)
    fifth = jax.random.fold_in(key, 15)
    groups = max(D // 64, 1)
    columns = D // groups
    scales = jnp.exp(jax.random.uniform(second, (STREAMS, TOKENS, groups, 1), jnp.float32, -1.2, 1.2))
    coarse = jnp.exp(jax.random.uniform(fifth, (STREAMS, TOKENS, 8, 1), jnp.float32, -1.5, 1.5))
    values = jax.random.normal(first, (STREAMS, TOKENS, groups, columns), jnp.float32) * scales
    values = values.reshape(STREAMS, TOKENS, 8, D // 8) * coarse
    return jnp.clip(values, -8.0, 8.0).reshape(STREAMS, TOKENS, D)


def steps_of(stream_key, dims, shards, least, high):
    level, own = 1.0, jax.random.fold_in(stream_key, 6)
    for dim, blocks in shards:
        steps = jnp.exp(jax.random.uniform(jax.random.fold_in(own, dim), (blocks,), jnp.float32, least / len(shards), high / len(shards)))
        level = level * jnp.repeat(steps, dims[dim] // blocks).reshape([-1 if axis == dim else 1 for axis in range(len(dims))])
    return level


def noise(own_key, shape, scale, bound, cuts=(), kind=jnp.bfloat16):
    array = scale * jax.random.normal(own_key, shape, jnp.float32)
    if cuts:
        array = array * steps_of(own_key, shape, cuts, -0.22, 0.18)
    return jnp.clip(array, -bound, bound).astype(kind)


def setup_inputs(seed: int = 0) -> dict:
    keys = jax.random.split(jax.random.key(seed), 9)
    return {
        "streams": draw_streams(jax.random.fold_in(keys[8], 71), 0),
        "mix_weight": noise(keys[1], (LOGITS, STREAMS, D), (STREAMS * D) ** -0.5, 0.046875, ((2, 4),), jnp.float32),
        "mix_bias": noise(keys[2], (LOGITS,), 1.0, 4.0, (), jnp.float32),
        "mix_scale": jnp.clip(jax.random.uniform(keys[3], (3,), jnp.float32, 1.0, 2.0), 1.0, 2.0),
        "norm_gain": jnp.clip(1.0 + 0.15 * jax.random.normal(keys[4], (D,), jnp.float32), 0.25, 1.75).astype(jnp.bfloat16),
        "gate_weight": noise(keys[5], (D, FF), D ** -0.5, 0.09375, ((0, 8), (1, 4))),
        "up_weight": noise(keys[6], (D, FF), D ** -0.5, 0.09375, ((0, 8), (1, 4))),
        "down_weight": noise(keys[7], (FF, D), FF ** -0.5, 0.0625, ((0, 4), (1, 8))),
    }


epsilon = 0.25

def coefficients(logits, mix_bias, mix_scale):
    pre_mix = jax.nn.sigmoid(mix_scale[0] * logits[:STREAMS] + mix_bias[:STREAMS, None])
    post_mix = 2.0 * jax.nn.sigmoid(mix_scale[1] * logits[STREAMS:2 * STREAMS] + mix_bias[STREAMS:2 * STREAMS, None])
    start_mix = jnp.exp(mix_scale[2] * logits[2 * STREAMS:] + mix_bias[2 * STREAMS:, None])
    start_mix = start_mix.reshape(STREAMS, STREAMS, logits.shape[1])

    def balance(iteration, matrix):
        matrix = matrix / lax.optimization_barrier(jnp.sum(matrix, axis=1, keepdims=True))
        return matrix / lax.optimization_barrier(jnp.sum(matrix, axis=0, keepdims=True))
    return (pre_mix, post_mix, lax.fori_loop(0, SWEEPS, balance, start_mix))

def layer_block(block, streams, mix_weight, mix_bias, mix_scale, norm_gain, gate_weight, up_weight, down_weight):
    current = lax.dynamic_slice_in_dim(streams, (block * TOK_DEV).astype(jnp.int32), TOK_DEV, 1)
    squares = lax.optimization_barrier(jnp.sum(current * current, axis=(0, 2)))
    inverse = lax.rsqrt(squares / (STREAMS * D) + epsilon)
    raw_logits = jnp.einsum('lkd,ktd->lt', mix_weight, current, precision=lax.Precision.HIGHEST)
    pre_mix, post_mix, res_mix = coefficients(raw_logits * inverse[None, :], mix_bias, mix_scale)
    layer_in = lax.optimization_barrier(jnp.sum(pre_mix[:, :, None] * current, axis=0)).astype(jnp.bfloat16)
    as_float = layer_in.astype(jnp.float32)
    mean_square = lax.optimization_barrier(jnp.mean(as_float * as_float, axis=1, keepdims=True))
    normed = (as_float * lax.rsqrt(mean_square + epsilon) * norm_gain.astype(jnp.float32)).astype(jnp.bfloat16)
    gate_value = jnp.dot(normed, gate_weight, preferred_element_type=jnp.float32)
    up_value = jnp.dot(normed, up_weight, preferred_element_type=jnp.float32)
    hidden = (jax.nn.silu(gate_value) * up_value).astype(jnp.bfloat16)
    share = FF // N_TENSOR
    layer_out = jnp.zeros((TOK_DEV, D), jnp.float32)
    for group in range(N_TENSOR):
        partial_out = jnp.dot(hidden[:, group * share:(group + 1) * share], down_weight[group * share:(group + 1) * share], preferred_element_type=jnp.float32)
        rounded = lax.optimization_barrier(partial_out.astype(jnp.bfloat16))
        layer_out = layer_out + rounded.astype(jnp.float32)
    outputs = []
    for target in range(STREAMS):
        mixed = post_mix[target][:, None] * layer_out
        for source in range(STREAMS):
            mixed = mixed + res_mix[target, source][:, None] * current[source]
        outputs.append(mixed)
    return jnp.stack(outputs)

def reference(streams, mix_weight, mix_bias, mix_scale, norm_gain, gate_weight, up_weight, down_weight):

    def one_block(block):
        return layer_block(block, streams, mix_weight, mix_bias, mix_scale, norm_gain, gate_weight, up_weight, down_weight)
    blocks = lax.map(one_block, jnp.arange(N_SEQ, dtype=jnp.int32))
    return jnp.moveaxis(blocks, 0, 1).reshape(STREAMS, TOKENS, D)
```

```python
import jax
import jax.numpy as jnp
from jax import lax
from jax.experimental import pallas as pl
from jax.experimental.pallas import tpu as pltpu
from jax.sharding import PartitionSpec as P

STREAMS = 4
SWEEPS = 20
CHUNKS = 2
EPSILON = 0.25


def coefficients(logits, mix_bias, mix_scale):
    pre_mix = jax.nn.sigmoid(mix_scale[0] * logits[:STREAMS] + mix_bias[:STREAMS, None])
    post_mix = 2.0 * jax.nn.sigmoid(
        mix_scale[1] * logits[STREAMS : 2 * STREAMS] + mix_bias[STREAMS : 2 * STREAMS, None]
    )
    start_mix = jnp.exp(mix_scale[2] * logits[2 * STREAMS :] + mix_bias[2 * STREAMS :, None])
    start_mix = start_mix.reshape(STREAMS, STREAMS, logits.shape[1])

    def balance(iteration, matrix):
        matrix = matrix / jnp.sum(matrix, axis=1, keepdims=True)
        return matrix / jnp.sum(matrix, axis=0, keepdims=True)

    return (pre_mix, post_mix, lax.fori_loop(0, SWEEPS, balance, start_mix))


def flip(value, axis, count, bit):
    return lax.ppermute(value, axis, [(i, i ^ bit) for i in range(count)])


def spread(value, count, bits, dim, after):
    offsets = [0]
    for bit in bits:
        other = flip(value, "seq", count, bit)
        if after is not None and len(offsets) == 1:
            other, _ = lax.optimization_barrier((other, after))
        value = lax.concatenate([value, other], dim)
        offsets = offsets + [o ^ bit for o in offsets]
    return value, offsets


def gather_halves(shard, count, dim, after=None):
    size = shard.shape[dim] // 2
    bits = []
    bit = 2
    while bit < count:
        bits.append(bit)
        bit *= 2
    pieces = []
    for half, order in ((0, bits), (1, bits[::-1])):
        part = lax.slice_in_dim(shard, half * size, (half + 1) * size, axis=dim)
        block, offsets = spread(part, count, order, dim, after)
        pieces.append((half, offsets, block))
        pieces.append((half, [o ^ 1 for o in offsets], flip(block, "seq", count, 1)))
    return pieces


def line_gather(block, count, me):
    right = [(i, i + 1) for i in range(count - 1)]
    left = [(i + 1, i) for i in range(count - 1)]
    from_left, from_right = [block], [block]
    for _ in range(count - 1):
        from_left.append(lax.ppermute(from_left[-1], "tensor", right))
        from_right.append(lax.ppermute(from_right[-1], "tensor", left))
    early = (from_left[max(count - 2, 1)], from_right[max(count - 2, 1)])
    return early, [block] + [
        jnp.where(me >= k, from_left[k], from_right[count - k]) for k in range(1, count)
    ]


def line_scatter(partial, count, me):
    def take(index):
        return lax.dynamic_index_in_dim(partial, jnp.clip(index, 0, count - 1), 0, keepdims=False)

    right = [(i, i + 1) for i in range(count - 1)]
    left = [(i + 1, i) for i in range(count - 1)]
    going_right = going_left = None
    for step in range(1, count):
        a, b = take(count - step + me), take(step - count + me)
        if step > 1:
            a = (a.astype(jnp.float32) + going_right.astype(jnp.float32)).astype(jnp.bfloat16)
            b = (b.astype(jnp.float32) + going_left.astype(jnp.float32)).astype(jnp.bfloat16)
        going_right = lax.ppermute(a, "tensor", right)
        going_left = lax.ppermute(b, "tensor", left)
    return (
        take(me).astype(jnp.float32)
        + going_right.astype(jnp.float32)
        + going_left.astype(jnp.float32)
    )


def mix_kernel(streams_ref, layer_ref, mix_ref, out_ref):
    layer_out = layer_ref[...]
    for target in range(STREAMS):
        mixed = mix_ref[:, target : target + 1] * layer_out
        for source in range(STREAMS):
            at = STREAMS * (1 + target) + source
            mixed = mixed + mix_ref[:, at : at + 1] * streams_ref[source]
        out_ref[target] = mixed


def mix_streams(streams, layer_out, post_mix, res_mix):
    tokens, width = layer_out.shape
    mixes = jnp.concatenate([post_mix, res_mix.reshape(STREAMS * STREAMS, tokens)]).T
    tile = 64
    return pl.pallas_call(
        mix_kernel,
        grid=(tokens // tile,),
        in_specs=[
            pl.BlockSpec((STREAMS, tile, width), lambda i: (0, i, 0)),
            pl.BlockSpec((tile, width), lambda i: (i, 0)),
            pl.BlockSpec((tile, mixes.shape[1]), lambda i: (i, 0)),
        ],
        out_specs=pl.BlockSpec((STREAMS, tile, width), lambda i: (0, i, 0)),
        out_shape=jax.ShapeDtypeStruct(streams.shape, jnp.float32),
        cost_estimate=pl.CostEstimate(
            flops=40 * tokens * width, bytes_accessed=36 * tokens * width, transcendentals=0
        ),
        compiler_params=pltpu.CompilerParams(vmem_limit_bytes=16 * 1024 * 1024),
    )(streams, layer_out, mixes)


def solution(mesh):
    n_seq, n_tensor = mesh.shape["seq"], mesh.shape["tensor"]

    def body(
        streams, mix_weight, mix_bias, mix_scale, norm_gain, gate_weight, up_weight, down_weight
    ):
        _, width = streams.shape[1:]
        features = width * n_tensor
        rows = features // n_seq
        seq, me = lax.axis_index("seq"), lax.axis_index("tensor")

        gate_parts = gather_halves(gate_weight, n_seq, 0)
        up_parts = gather_halves(up_weight, n_seq, 0)

        squares = jnp.sum(streams * streams, axis=(0, 2))[None, :]
        raw_logits = jnp.einsum("lkd,ktd->lt", mix_weight, streams, precision=lax.Precision.HIGHEST)
        own = jnp.concatenate([raw_logits, squares])
        total = own
        for shift in range(1, n_tensor):
            total = total + lax.ppermute(
                own, "tensor", [(i, (i + shift) % n_tensor) for i in range(n_tensor)]
            )
        logits = total[:-1] * lax.rsqrt(total[-1:] / (STREAMS * features) + EPSILON)
        pre_mix, post_mix, res_mix = coefficients(logits, mix_bias, mix_scale)
        layer_in = jnp.sum(pre_mix[:, :, None] * streams, axis=0).astype(jnp.bfloat16)

        early, blocks = line_gather(layer_in, n_tensor, me)
        relative = jnp.stack(blocks)
        arrived = tuple(part[2][-8:, :128] for part in (*gate_parts[::2], *up_parts[::2]))
        down_shard, _ = lax.optimization_barrier((down_weight, early))
        chunk = down_shard.shape[1] // CHUNKS
        down_parts = [
            gather_halves(down_shard[:, c * chunk : (c + 1) * chunk], n_seq, 1, arrived)
            for c in range(CHUNKS)
        ]
        whole_input = jnp.concatenate(
            [
                lax.dynamic_index_in_dim(relative, (me - b) % n_tensor, 0, keepdims=False)
                for b in range(n_tensor)
            ],
            axis=1,
        )
        as_float = whole_input.astype(jnp.float32)
        mean_square = jnp.mean(as_float * as_float, axis=1, keepdims=True)
        normed = (
            as_float * lax.rsqrt(mean_square + EPSILON) * norm_gain.astype(jnp.float32)
        ).astype(jnp.bfloat16)

        def rows_of(half, offsets):
            size = rows // 2
            return jnp.concatenate(
                [
                    lax.dynamic_slice_in_dim(normed, (seq ^ o) * rows + half * size, size, 1)
                    for o in offsets
                ],
                axis=1,
            )

        gate_value = up_value = 0.0
        for (half, offsets, gate_block), (_, _, up_block) in zip(gate_parts, up_parts):
            part = rows_of(half, offsets)
            gate_value += jnp.dot(part, gate_block, preferred_element_type=jnp.float32)
            up_value += jnp.dot(part, up_block, preferred_element_type=jnp.float32)
        hidden = (jax.nn.silu(gate_value) * up_value).astype(jnp.bfloat16)

        per, size = n_seq // n_tensor, chunk // 2
        scattered = []
        for parts in down_parts:
            quarters = {0: [None] * n_seq, 1: [None] * n_seq}
            for half, offsets, block in parts:
                product = jnp.dot(hidden, block, preferred_element_type=jnp.float32)
                product = product.astype(jnp.bfloat16)
                for i, o in enumerate(offsets):
                    quarters[half][o] = product[:, i * size : (i + 1) * size]
            stack = jnp.stack(
                [jnp.concatenate([quarters[0][o], quarters[1][o]], axis=1) for o in range(n_seq)]
            )

            order = [
                lax.dynamic_index_in_dim(stack, seq ^ o, 0, keepdims=False) for o in range(n_seq)
            ]
            partial = jnp.stack(
                [
                    jnp.concatenate(order[d * per : (d + 1) * per], axis=1)
                    for d in range(n_tensor)
                ]
            )
            scattered.append(line_scatter(partial, n_tensor, me))
        layer_out = jnp.concatenate(
            [part[:, p * chunk : (p + 1) * chunk] for p in range(per) for part in scattered],
            axis=1,
        )
        return mix_streams(streams, layer_out, post_mix, res_mix)

    placed = (
        P(None, "seq", "tensor"),
        P(None, None, "tensor"),
        P(),
        P(),
        P(),
        P("seq", "tensor"),
        P("seq", "tensor"),
        P("tensor", "seq"),
    )

    return jax.shard_map(
        body, mesh=mesh, in_specs=placed, out_specs=P(None, "seq", "tensor"), check_vma=False
    )
```

```python
import jax
import jax.numpy as jnp
from jax import lax
from jax.experimental import pallas as pl
from jax.experimental.pallas import tpu as pltpu
from jax.sharding import PartitionSpec as P

STREAMS = 4
SWEEPS = 20
CHUNKS = 2
EPSILON = 0.25


def coefficients(logits, mix_bias, mix_scale):
    pre_mix = jax.nn.sigmoid(mix_scale[0] * logits[:STREAMS] + mix_bias[:STREAMS, None])
    post_mix = 2.0 * jax.nn.sigmoid(
        mix_scale[1] * logits[STREAMS : 2 * STREAMS] + mix_bias[STREAMS : 2 * STREAMS, None]
    )
    start_mix = jnp.exp(mix_scale[2] * logits[2 * STREAMS :] + mix_bias[2 * STREAMS :, None])
    start_mix = start_mix.reshape(STREAMS, STREAMS, logits.shape[1])

    def balance(iteration, matrix):
        matrix = matrix / jnp.sum(matrix, axis=1, keepdims=True)
        return matrix / jnp.sum(matrix, axis=0, keepdims=True)

    return (pre_mix, post_mix, lax.fori_loop(0, SWEEPS, balance, start_mix))


def flip(value, axis, count, bit):
    return lax.ppermute(value, axis, [(i, i ^ bit) for i in range(count)])


def spread(value, count, bits, dim, after, late):
    offsets = [0]
    for bit in bits:
        other = flip(value, "seq", count, bit)
        if after is not None and len(offsets) == 1:
            other, _ = lax.optimization_barrier((other, after))
        if late is not None and bit == bits[-1]:
            other, _ = lax.optimization_barrier((other, late))
        value = lax.concatenate([value, other], dim)
        offsets = offsets + [o ^ bit for o in offsets]
    return value, offsets


def gather_halves(shard, count, dim, after=None, late=None):
    size = shard.shape[dim] // 2
    bits = []
    bit = 2
    while bit < count:
        bits.append(bit)
        bit *= 2
    pieces = []
    for half, order in ((0, bits), (1, bits[::-1])):
        part = lax.slice_in_dim(shard, half * size, (half + 1) * size, axis=dim)
        block, offsets = spread(part, count, order, dim, after, late)
        pieces.append((half, offsets, block))
        pieces.append((half, [o ^ 1 for o in offsets], flip(block, "seq", count, 1)))
    return pieces


def line_gather(block, count, me):
    right = [(i, i + 1) for i in range(count - 1)]
    left = [(i + 1, i) for i in range(count - 1)]
    from_left, from_right = [block], [block]
    for _ in range(count - 1):
        from_left.append(lax.ppermute(from_left[-1], "tensor", right))
        from_right.append(lax.ppermute(from_right[-1], "tensor", left))
    early = (from_left[max(count - 2, 1)], from_right[max(count - 2, 1)])
    last = (from_left[-1][-8:, -128:], from_right[-1][-8:, -128:])
    return early, last, [block] + [
        jnp.where(me >= k, from_left[k], from_right[count - k]) for k in range(1, count)
    ]


def line_scatter(take, count, me):
    right = [(i, i + 1) for i in range(count - 1)]
    left = [(i + 1, i) for i in range(count - 1)]
    going_right = going_left = None
    for step in range(1, count):
        a, b = take(count - step + me), take(step - count + me)
        if step > 1:
            a = (a.astype(jnp.float32) + going_right.astype(jnp.float32)).astype(jnp.bfloat16)
            b = (b.astype(jnp.float32) + going_left.astype(jnp.float32)).astype(jnp.bfloat16)
        going_right = lax.ppermute(a, "tensor", right)
        going_left = lax.ppermute(b, "tensor", left)
    return (
        take(me).astype(jnp.float32)
        + going_right.astype(jnp.float32)
        + going_left.astype(jnp.float32)
    )


def mix_kernel(streams_ref, layer_ref, mix_ref, out_ref):
    layer_out = layer_ref[...]
    for target in range(STREAMS):
        mixed = mix_ref[:, target : target + 1] * layer_out
        for source in range(STREAMS):
            at = STREAMS * (1 + target) + source
            mixed = mixed + mix_ref[:, at : at + 1] * streams_ref[source]
        out_ref[target] = mixed


def mix_streams(streams, layer_out, post_mix, res_mix):
    tokens, width = layer_out.shape
    mixes = jnp.concatenate([post_mix, res_mix.reshape(STREAMS * STREAMS, tokens)]).T
    tile = 64
    return pl.pallas_call(
        mix_kernel,
        grid=(tokens // tile,),
        in_specs=[
            pl.BlockSpec((STREAMS, tile, width), lambda i: (0, i, 0)),
            pl.BlockSpec((tile, width), lambda i: (i, 0)),
            pl.BlockSpec((tile, mixes.shape[1]), lambda i: (i, 0)),
        ],
        out_specs=pl.BlockSpec((STREAMS, tile, width), lambda i: (0, i, 0)),
        out_shape=jax.ShapeDtypeStruct(streams.shape, jnp.float32),
        cost_estimate=pl.CostEstimate(
            flops=40 * tokens * width, bytes_accessed=36 * tokens * width, transcendentals=0
        ),
        compiler_params=pltpu.CompilerParams(vmem_limit_bytes=16 * 1024 * 1024),
    )(streams, layer_out, mixes)


def solution(mesh):
    n_seq, n_tensor = mesh.shape["seq"], mesh.shape["tensor"]

    def body(
        streams, mix_weight, mix_bias, mix_scale, norm_gain, gate_weight, up_weight, down_weight
    ):
        _, width = streams.shape[1:]
        features = width * n_tensor
        rows = features // n_seq
        seq, me = lax.axis_index("seq"), lax.axis_index("tensor")

        gate_parts = gather_halves(gate_weight, n_seq, 0)

        squares = jnp.sum(streams * streams, axis=(0, 2))[None, :]
        raw_logits = jnp.einsum("lkd,ktd->lt", mix_weight, streams, precision=lax.Precision.HIGHEST)
        own = jnp.concatenate([raw_logits, squares])
        total = own
        for shift in range(1, n_tensor):
            total = total + lax.ppermute(
                own, "tensor", [(i, (i + shift) % n_tensor) for i in range(n_tensor)]
            )
        logits = total[:-1] * lax.rsqrt(total[-1:] / (STREAMS * features) + EPSILON)
        pre_mix, post_mix, res_mix = coefficients(logits, mix_bias, mix_scale)
        layer_in = jnp.sum(pre_mix[:, :, None] * streams, axis=0).astype(jnp.bfloat16)

        early, last, blocks = line_gather(layer_in, n_tensor, me)
        relative = jnp.stack(blocks)
        up_parts = gather_halves(up_weight, n_seq, 0, late=last)
        arrived = tuple(part[2][-8:, :128] for part in (*gate_parts[::2], *up_parts[::2]))
        down_shard, _ = lax.optimization_barrier((down_weight, early))
        chunk = down_shard.shape[1] // CHUNKS
        down_parts = [
            gather_halves(down_shard[:, c * chunk : (c + 1) * chunk], n_seq, 1, arrived)
            for c in range(CHUNKS)
        ]
        whole_input = jnp.concatenate(
            [
                lax.dynamic_index_in_dim(relative, (me - b) % n_tensor, 0, keepdims=False)
                for b in range(n_tensor)
            ],
            axis=1,
        )
        as_float = whole_input.astype(jnp.float32)
        mean_square = jnp.mean(as_float * as_float, axis=1, keepdims=True)
        normed = (
            as_float * lax.rsqrt(mean_square + EPSILON) * norm_gain.astype(jnp.float32)
        ).astype(jnp.bfloat16)

        def rows_of(half, offsets):
            size = rows // 2
            return jnp.concatenate(
                [
                    lax.dynamic_slice_in_dim(normed, (seq ^ o) * rows + half * size, size, 1)
                    for o in offsets
                ],
                axis=1,
            )

        gate_value = up_value = 0.0
        for (half, offsets, gate_block), (_, _, up_block) in zip(gate_parts, up_parts):
            part = rows_of(half, offsets)
            gate_value += jnp.dot(part, gate_block, preferred_element_type=jnp.float32)
            up_value += jnp.dot(part, up_block, preferred_element_type=jnp.float32)
        hidden = (jax.nn.silu(gate_value) * up_value).astype(jnp.bfloat16)

        per, size = n_seq // n_tensor, chunk // 2
        scattered, ready = [], hidden
        for c, parts in enumerate(down_parts):
            products, places = [], {0: [0] * n_seq, 1: [0] * n_seq}
            for half, offsets, block in parts:
                for o in offsets:
                    places[half][o] = len(products) * len(offsets) * size
                    places[half][o] += offsets.index(o) * size
                product = jnp.dot(ready, block, preferred_element_type=jnp.float32)
                products.append(product.astype(jnp.bfloat16))
            wide = jnp.concatenate(products, axis=1)
            tables = [jnp.array(places[half], jnp.int32) for half in (0, 1)]

            def take(index, wide=wide, tables=tables):
                start = jnp.clip(index, 0, n_tensor - 1) * per
                return jnp.concatenate(
                    [
                        lax.dynamic_slice_in_dim(wide, tables[half][seq ^ (start + p)], size, 1)
                        for p in range(per)
                        for half in (0, 1)
                    ],
                    axis=1,
                )

            if c + 1 < CHUNKS:
                ready, _ = lax.optimization_barrier((hidden, take(n_tensor - 1 + me)))
            scattered.append(line_scatter(take, n_tensor, me))
        layer_out = jnp.concatenate(
            [part[:, p * chunk : (p + 1) * chunk] for p in range(per) for part in scattered],
            axis=1,
        )
        return mix_streams(streams, layer_out, post_mix, res_mix)

    placed = (
        P(None, "seq", "tensor"),
        P(None, None, "tensor"),
        P(),
        P(),
        P(),
        P("seq", "tensor"),
        P("seq", "tensor"),
        P("tensor", "seq"),
    )

    return jax.shard_map(
        body, mesh=mesh, in_specs=placed, out_specs=P(None, "seq", "tensor"), check_vma=False
    )
```
